512 devices in a mesh: blk: 128 (over y, x, z_hi), sub: 4 (over z_lo, core).
Axes of the slice: x: 4, y: 8, z: 8 (z_hi: 4, z_lo: 2; z = z_hi * 2 + z_lo), core: 2. Of those that a mesh axis runs over, the one named last changes fastest.
Arguments:
- first_core: bfloat16 [128, 128], P('blk'), may hold values from -6 to 6
- middle_core: bfloat16 [32, 32, 256], P(None, 'sub'), may hold values from -1 to 1
- last_core: bfloat16 [32, 512], replicated, may hold values from -1 to 1
- row_tt: int32 [524288], P(('blk', 'sub')), may hold values from 0 to 524287, as said below
Outputs:
- served: bfloat16 [524288, 128], P(('blk', 'sub'))
The draws below stay inside these ranges and needn't reach their ends.
Inputs may be any that keep to these rules, and one draw needn't show every extreme that they name: `row_tt`: each window row is named exactly once. Among the rows of one device, exactly 2 entries lie in each of the 512 ranges q * 1024 to (q + 1) * 1024 - 1.
All inputs are finite; a program needn't handle non-finite values.
Results may differ from the reference program's by a relative error of at most 0.0049.
Values may be sent and summed in bfloat16 or wider, within the bound.
No kernel may reach another device: no remote copies, remote signals or barrier semaphores. Data moves between devices by JAX's collectives and lax.ppermute only.
A program may use at most 64 MiB of HBM per device.

```python
import jax
import jax.numpy as jnp
from jax import lax

R = 32
J1 = 4
J2 = 8
J3 = 4
W3 = 128
NI1 = 128
I2W = 32
ROWS_DEV = 1024
SOURCES = 512
PEER = 2


def draw_row_tt(key, part):
    spread_keys = jax.random.split(jax.random.fold_in(key, 11), SOURCES)
    spread = jax.vmap(lambda subkey: jax.random.permutation(subkey, ROWS_DEV))(spread_keys)
    spread = spread.astype(jnp.int32).reshape(SOURCES, SOURCES, PEER).transpose(1, 0, 2)
    owner_id = jnp.arange(SOURCES, dtype=jnp.int32)[None, :, None]
    flat_index = (owner_id * ROWS_DEV + spread).reshape(SOURCES, ROWS_DEV)
    shuffle_keys = jax.random.split(jax.random.fold_in(key, 12), SOURCES)
    shuffled = jax.vmap(lambda subkey, row_list: jax.random.permutation(subkey, row_list))(shuffle_keys, flat_index)
    return shuffled.reshape(-1).astype(jnp.int32)


def block_scale(stream_key, dims, cuts, least, top_value):
    def one(position, shards_of):
        draws = jax.random.uniform(jax.random.fold_in(jax.random.fold_in(stream_key, 6), position), (shards_of,), jnp.float32, least / len(cuts), top_value / len(cuts))
        return jnp.repeat(jnp.exp(draws), dims[position] // shards_of).reshape((-1,) + (1,) * (len(dims) - position - 1))

    gain = one(*cuts[0])
    for cut in cuts[1:]:
        gain = gain * one(*cut)
    return gain


def scatter_about(key, dims, scale, reach, shards=(), held_as=jnp.bfloat16):
    array = jax.random.normal(key, dims, jnp.float32) * scale
    if len(shards) > 0:
        array = block_scale(key, dims, shards, -0.22, 0.18) * array
    return jnp.clip(array, min=-reach, max=reach).astype(held_as)


def setup_inputs(seed: int = 0) -> dict:
    splits = jax.random.split(jax.random.key(seed), 5)
    return {
        "first_core": scatter_about(splits[0], (NI1, J1 * R), 1.0, 6.0, ((0, 128),)),
        "middle_core": scatter_about(splits[1], (R, I2W, J2 * R), R ** -0.5, 1.0, ((1, 4),)),
        "last_core": scatter_about(splits[2], (R, W3 * J3), R ** -0.5, 1.0),
        "row_tt": draw_row_tt(jax.random.fold_in(splits[4], 71), 0),
    }


def reference(first_core, middle_core, last_core, row_tt):
    middle_span = middle_core.shape[1]
    last_span = last_core.shape[1] // J3
    flat_middle = middle_core.reshape(R, middle_span * J2 * R)

    def slab_of(first_row):
        partial_value = jnp.dot(first_row.reshape(J1, R), flat_middle, preferred_element_type=jnp.float32).astype(jnp.bfloat16)
        partial_value = partial_value.reshape(J1, middle_span, J2, R).transpose(1, 0, 2, 3).reshape(middle_span * J1 * J2, R)
        products = jnp.dot(partial_value, last_core, preferred_element_type=jnp.float32).astype(jnp.bfloat16)
        products = products.reshape(middle_span, J1, J2, last_span, J3).transpose(0, 3, 1, 2, 4)
        return products.reshape(middle_span * last_span, J1 * J2 * J3)

    table = lax.map(slab_of, first_core)
    table = table.reshape(-1, J1 * J2 * J3)
    return jnp.take(table, row_tt.astype(jnp.int32), axis=0)
```

```python
import jax
import jax.numpy as jnp
from jax import lax
from jax.experimental import pallas as pl
from jax.experimental.pallas import tpu as pltpu
from jax.sharding import PartitionSpec as P


R = 32
J1 = 4
J2 = 8
J3 = 4
W3 = 128
I2L = 8
GROUPS = 4
ROWS = 1024
KT = 256


def mid_last_kernel(zlo_ref, row_ref, mid_ref, last_ref, q_ref, w_ref, b_ref, y_ref):
    f32, bf16 = jnp.float32, jnp.bfloat16
    shape3 = (R, I2L, J2 * R)
    sub_i = lax.broadcasted_iota(jnp.int32, shape3, 1)
    lane_i = lax.broadcasted_iota(jnp.int32, shape3, 2)
    for t in range(GROUPS):
        x = mid_ref[pl.ds(t * 256, 256), :].astype(f32).reshape(shape3)
        for bit in range(3):
            rb = (sub_i >> bit) & 1
            lb = (lane_i >> (5 + bit)) & 1
            step, span = 1 << bit, R << bit
            up = pltpu.roll(pltpu.roll(x, 8 - step, 1), span, 2)
            down = pltpu.roll(pltpu.roll(x, step, 1), 256 - span, 2)
            x = jnp.where(rb == lb, x, jnp.where(rb == 0, up, down))
        w_ref[:, pl.ds(t * 256, 256)] = x.reshape(256, 256).astype(bf16)
    c_i = lax.broadcasted_iota(jnp.int32, (512, 512), 0)
    d_i = lax.broadcasted_iota(jnp.int32, (512, 512), 1)
    pick = jnp.where(c_i == (d_i & 127) * J3 + (d_i >> 7), 1.0, 0.0).astype(bf16)
    spread = jnp.dot(last_ref[...], pick, preferred_element_type=f32).astype(bf16)
    stacked = jnp.concatenate([spread[:, j * W3 : (j + 1) * W3] for j in range(J3)], axis=0)
    row = row_ref[...]
    i3 = row & (W3 - 1)
    hot3 = jnp.where(lax.broadcasted_iota(jnp.int32, (W3, ROWS), 0) == i3, 1.0, 0.0).astype(bf16)
    b_ref[...] = jnp.dot(stacked, hot3, preferred_element_type=f32).astype(bf16)
    group = (row >> 10) & 3
    slot = ((group & 1) << 1) | ((group >> 1) ^ zlo_ref[0])
    code_all = slot * I2L + ((row >> 7) & (I2L - 1))
    for kt in range(ROWS // KT):
        ks = pl.ds(kt * KT, KT)
        code = jnp.broadcast_to(code_all[:, kt * KT : (kt + 1) * KT], (R, KT))
        for c in range(GROUPS * I2L):
            mask = jnp.where(code == c, 1.0, 0.0).astype(bf16)
            for j in range(J3):
                y_ref[j, pl.ds(c * R, R), :] = b_ref[pl.ds(j * R, R), ks] * mask
        for j in range(J3):
            q_ref[j, :, ks] = jnp.dot(w_ref[...], y_ref[j], preferred_element_type=f32).astype(bf16)


def first_kernel(row_ref, first_ref, q_ref, out_ref, a_ref, t_ref):
    f32, bf16 = jnp.float32, jnp.bfloat16
    blocks = first_ref.shape[0]
    i1 = row_ref[...] >> 12
    hot1 = jnp.where(lax.broadcasted_iota(jnp.int32, (blocks, ROWS), 0) == i1, 1.0, 0.0).astype(bf16)
    a_ref[...] = lax.dot_general(
        first_ref[...], hot1, (((0,), (0,)), ((), ())), preferred_element_type=f32
    )

    def tile(kt, carry):
        ks = pl.ds(pl.multiple_of(kt * 128, 128), 128)
        acc = [[None] * J3 for _ in range(J1)]
        for r in range(0, R, 2):
            for j3 in range(J3):
                both = q_ref[j3, pl.ds(r * J2, 2 * J2), ks].astype(f32)
                for h in range(2):
                    q = both[h * J2 : (h + 1) * J2]
                    for j1 in range(J1):
                        term = a_ref[pl.ds(j1 * R + r + h, 1), ks] * q
                        acc[j1][j3] = term if acc[j1][j3] is None else acc[j1][j3] + term
        for j1 in range(J1):
            for j3 in range(J3):
                t_ref[pl.ds(j1 * J2 * J3 + j3, J2, stride=J3), :] = acc[j1][j3]
        out_ref[ks, :] = t_ref[...].T.astype(bf16)
        return carry

    lax.fori_loop(0, ROWS // 128, tile, 0)


def served_rows(first_core, middle_core, last_core, row_tt):
    blocks = lax.axis_size("blk")
    groups = lax.axis_size("sub")
    vmem = pl.BlockSpec(memory_space=pltpu.VMEM)
    row = row_tt.reshape(1, ROWS)
    zlo = (lax.axis_index("sub") // 2).astype(jnp.int32).reshape(1)
    mid = middle_core.reshape(R * I2L, J2 * R)
    other = lax.ppermute(mid, "sub", [(i, i ^ 2) for i in range(groups)])
    sent = jnp.broadcast_to(first_core, (blocks, J1 * R))
    first_all = lax.all_to_all(sent, "blk", split_axis=0, concat_axis=0, tiled=True)
    pair = jnp.concatenate([mid, other], axis=0)
    mid_all = lax.all_gather(pair, "sub", axis_index_groups=[[0, 1], [2, 3]], tiled=True)
    q = early_call(zlo, row, mid_all, last_core, vmem)
    return late_call(row, first_all, q, vmem)


def early_call(zlo, row, mid_all, last_core, vmem):
    return pl.pallas_call(
        mid_last_kernel,
        out_shape=jax.ShapeDtypeStruct((J3, R * J2, ROWS), jnp.bfloat16),
        in_specs=[pl.BlockSpec(memory_space=pltpu.SMEM), vmem, vmem, vmem],
        out_specs=vmem,
        scratch_shapes=[
            pltpu.VMEM((R * J2, GROUPS * I2L * R), jnp.bfloat16),
            pltpu.VMEM((J3 * R, ROWS), jnp.bfloat16),
            pltpu.VMEM((J3, GROUPS * I2L * R, KT), jnp.bfloat16),
        ],
        compiler_params=pltpu.CompilerParams(vmem_limit_bytes=24 * 1024 * 1024),
        name="mid_last",
    )(zlo, row, mid_all, last_core)


def late_call(row, first_all, q, vmem):
    return pl.pallas_call(
        first_kernel,
        out_shape=jax.ShapeDtypeStruct((ROWS, J1 * J2 * J3), jnp.bfloat16),
        in_specs=[vmem, vmem, vmem],
        out_specs=vmem,
        scratch_shapes=[
            pltpu.VMEM((J1 * R, ROWS), jnp.float32),
            pltpu.VMEM((J1 * J2 * J3, 128), jnp.float32),
        ],
        compiler_params=pltpu.CompilerParams(vmem_limit_bytes=24 * 1024 * 1024),
        name="first",
    )(row, first_all, q)


def solution(mesh):
    placed = (P("blk", None), P(None, "sub", None), P(), P(("blk", "sub")))
    return jax.shard_map(
        served_rows, mesh=mesh, in_specs=placed, out_specs=P(("blk", "sub"), None), check_vma=False
    )
```

```python
import jax
import jax.numpy as jnp
from jax import lax
from jax.experimental import pallas as pl
from jax.experimental.pallas import tpu as pltpu
from jax.sharding import PartitionSpec as P


R = 32
J1 = 4
J2 = 8
J3 = 4
W3 = 128
I2L = 8
GROUPS = 4
ROWS = 1024
KT = 256


def mid_last_kernel(row_hbm, mid_ref, last_hbm, q_ref, w_ref, b_ref, y_ref, row_ref, last_ref, sems):
    f32, bf16 = jnp.float32, jnp.bfloat16
    get_row = pltpu.make_async_copy(row_hbm, row_ref, sems.at[0])
    get_last = pltpu.make_async_copy(last_hbm, last_ref, sems.at[1])
    get_row.start()
    get_last.start()
    shape3 = (R, I2L, J2 * R)
    sub_i = lax.broadcasted_iota(jnp.int32, shape3, 1)
    lane_i = lax.broadcasted_iota(jnp.int32, shape3, 2)
    for t in range(GROUPS):
        x = mid_ref[pl.ds(t * 256, 256), :].astype(f32).reshape(shape3)
        for bit in range(3):
            rb = (sub_i >> bit) & 1
            lb = (lane_i >> (5 + bit)) & 1
            step, span = 1 << bit, R << bit
            up = pltpu.roll(pltpu.roll(x, 8 - step, 1), span, 2)
            down = pltpu.roll(pltpu.roll(x, step, 1), 256 - span, 2)
            x = jnp.where(rb == lb, x, jnp.where(rb == 0, up, down))
        w_ref[:, pl.ds(t * 256, 256)] = x.reshape(256, 256).astype(bf16)
    get_row.wait()
    get_last.wait()
    c_i = lax.broadcasted_iota(jnp.int32, (512, 512), 0)
    d_i = lax.broadcasted_iota(jnp.int32, (512, 512), 1)
    pick = jnp.where(c_i == (d_i & 127) * J3 + (d_i >> 7), 1.0, 0.0).astype(bf16)
    spread = jnp.dot(last_ref[...], pick, preferred_element_type=f32).astype(bf16)
    stacked = jnp.concatenate([spread[:, j * W3 : (j + 1) * W3] for j in range(J3)], axis=0)
    row = row_ref[...]
    i3 = row & (W3 - 1)
    hot3 = jnp.where(lax.broadcasted_iota(jnp.int32, (W3, ROWS), 0) == i3, 1.0, 0.0).astype(bf16)
    b_ref[...] = jnp.dot(stacked, hot3, preferred_element_type=f32).astype(bf16)
    code_all = (row >> 7) & (GROUPS * I2L - 1)
    for kt in range(ROWS // KT):
        ks = pl.ds(kt * KT, KT)
        code = jnp.broadcast_to(code_all[:, kt * KT : (kt + 1) * KT], (R, KT))
        for c in range(GROUPS * I2L):
            mask = jnp.where(code == c, 1.0, 0.0).astype(bf16)
            for j in range(J3):
                y_ref[j, pl.ds(c * R, R), :] = b_ref[pl.ds(j * R, R), ks] * mask
        for j in range(J3):
            q_ref[j, :, ks] = jnp.dot(w_ref[...], y_ref[j], preferred_element_type=f32).astype(bf16)


def first_kernel(row_ref, first_ref, q_ref, out_ref, a_ref, t_ref, o_ref, sem):
    f32, bf16 = jnp.float32, jnp.bfloat16
    blocks = first_ref.shape[0]
    i1 = row_ref[...] >> 12
    hot1 = jnp.where(lax.broadcasted_iota(jnp.int32, (blocks, ROWS), 0) == i1, 1.0, 0.0).astype(bf16)
    a_ref[...] = lax.dot_general(
        first_ref[...], hot1, (((0,), (0,)), ((), ())), preferred_element_type=f32
    )

    def put(kt):
        ks = pl.ds(kt * 128, 128)
        return pltpu.make_async_copy(o_ref.at[ks], out_ref.at[ks], sem.at[kt])

    def tiles(step, carry):
        for u in range(8):
            kt = step * 8 + u
            ks = pl.ds(kt * 128, 128)
            acc = [[None] * J3 for _ in range(J1)]
            for r in range(0, R, 2):
                for j3 in range(J3):
                    both = q_ref[j3, pl.ds(r * J2, 2 * J2), ks].astype(f32)
                    for h in range(2):
                        q = both[h * J2 : (h + 1) * J2]
                        for j1 in range(J1):
                            term = a_ref[pl.ds(j1 * R + r + h, 1), ks] * q
                            acc[j1][j3] = term if acc[j1][j3] is None else acc[j1][j3] + term
            for j1 in range(J1):
                for j3 in range(J3):
                    t_ref[u, pl.ds(j1 * J2 * J3 + j3, J2, stride=J3), :] = acc[j1][j3]
            o_ref[ks, :] = t_ref[u].T.astype(bf16)
            put(kt).start()
        return carry

    tiles(0, 0)
    for kt in range(ROWS // 128):
        put(kt).wait()


def served_rows(first_core, middle_core, last_core, row_tt):
    blocks = lax.axis_size("blk")
    vmem = pl.BlockSpec(memory_space=pltpu.VMEM)
    row = row_tt.reshape(1, ROWS)
    mid = middle_core.reshape(R * I2L, J2 * R)
    sent = jnp.broadcast_to(first_core, (blocks, J1 * R))
    first_all = lax.all_to_all(sent, "blk", split_axis=0, concat_axis=0, tiled=True)
    mid_all = lax.all_gather(mid, "sub", tiled=True)
    q = early_call(row, mid_all, last_core, vmem)
    return late_call(row, first_all, q, vmem)


def early_call(row, mid_all, last_core, vmem):
    anywhere = pl.BlockSpec(memory_space=pltpu.HBM)
    return pl.pallas_call(
        mid_last_kernel,
        out_shape=jax.ShapeDtypeStruct((J3, R * J2, ROWS), jnp.bfloat16),
        in_specs=[anywhere, vmem, anywhere],
        out_specs=vmem,
        scratch_shapes=[
            pltpu.VMEM((R * J2, GROUPS * I2L * R), jnp.bfloat16),
            pltpu.VMEM((J3 * R, ROWS), jnp.bfloat16),
            pltpu.VMEM((J3, GROUPS * I2L * R, KT), jnp.bfloat16),
            pltpu.VMEM((1, ROWS), jnp.int32),
            pltpu.VMEM((R, W3 * J3), jnp.bfloat16),
            pltpu.SemaphoreType.DMA((2,)),
        ],
        compiler_params=pltpu.CompilerParams(vmem_limit_bytes=24 * 1024 * 1024),
        name="mid_last",
    )(
        pltpu.with_memory_space_constraint(row, pltpu.HBM),
        mid_all,
        pltpu.with_memory_space_constraint(last_core, pltpu.HBM),
    )


def late_call(row, first_all, q, vmem):
    return pl.pallas_call(
        first_kernel,
        out_shape=jax.ShapeDtypeStruct((ROWS, J1 * J2 * J3), jnp.bfloat16),
        in_specs=[vmem, vmem, vmem],
        out_specs=pl.BlockSpec(memory_space=pl.ANY),
        scratch_shapes=[
            pltpu.VMEM((J1 * R, ROWS), jnp.float32),
            pltpu.VMEM((8, J1 * J2 * J3, 128), jnp.float32),
            pltpu.VMEM((ROWS, J1 * J2 * J3), jnp.bfloat16),
            pltpu.SemaphoreType.DMA((ROWS // 128,)),
        ],
        compiler_params=pltpu.CompilerParams(vmem_limit_bytes=24 * 1024 * 1024),
        name="first",
    )(row, first_all, q)


def solution(mesh):
    placed = (P("blk", None), P(None, "sub", None), P(), P(("blk", "sub")))
    return jax.shard_map(
        served_rows, mesh=mesh, in_specs=placed, out_specs=P(("blk", "sub"), None), check_vma=False
    )
```

```python
import jax
import jax.numpy as jnp
from jax import lax
from jax.experimental import pallas as pl
from jax.experimental.pallas import tpu as pltpu
from jax.sharding import PartitionSpec as P


R = 32
J1 = 4
J2 = 8
J3 = 4
W3 = 128
I2L = 8
GROUPS = 4
ROWS = 1024
KT = 256
LEAD = 75
SOON = 6


def mid_last_kernel(
    order_ref, row_ref, mid_ref, last_ref, q_ref,
    w_ref, b_ref, y_ref, x_ref, v_ref,
):
    f32, bf16 = jnp.float32, jnp.bfloat16
    chunk = lax.broadcasted_iota(jnp.int32, (R, 128), 1) // R
    for t in range(GROUPS):
        for hj in range(2):
            x_ref[hj] = mid_ref[pl.ds(t * 256, 256), pl.ds(hj * 128, 128)].astype(f32)
        for hi in range(2):
            for hj in range(2):
                turned = []
                for i in range(4):
                    v = x_ref[hj, pl.ds(hi * 4 + i, R, stride=I2L), :]
                    turned.append([v] + [pltpu.roll(v, R * d, 1) for d in range(1, 4)])
                for j in range(4):
                    out = turned[0][(0 - j) % 4]
                    for i in range(1, 4):
                        out = jnp.where(chunk == i, turned[i][(i - j) % 4], out)
                    v_ref[hi, pl.ds(hj * 4 + j, R, stride=J2), :] = out
        for hi in range(2):
            w_ref[:, pl.ds(t * 256 + hi * 128, 128)] = v_ref[hi].astype(bf16)
    c_i = lax.broadcasted_iota(jnp.int32, (512, 512), 0)
    d_i = lax.broadcasted_iota(jnp.int32, (512, 512), 1)
    pick = jnp.where(c_i == (d_i & 127) * J3 + (d_i >> 7), 1.0, 0.0).astype(bf16)
    spread = jnp.dot(last_ref[...], pick, preferred_element_type=f32).astype(bf16)
    stacked = jnp.concatenate([spread[:, j * W3 : (j + 1) * W3] for j in range(J3)], axis=0)
    row = row_ref[...]
    i3 = row & (W3 - 1)
    hot3 = jnp.where(lax.broadcasted_iota(jnp.int32, (W3, ROWS), 0) == i3, 1.0, 0.0).astype(bf16)
    b_ref[...] = jnp.dot(stacked, hot3, preferred_element_type=f32).astype(bf16)
    group = (row >> 10) & 3
    paired = ((group & 1) << 1) | ((group >> 1) ^ order_ref[1])
    slot = jnp.where(order_ref[0] == 1, paired, group)
    code_all = slot * I2L + ((row >> 7) & (I2L - 1))
    for kt in range(ROWS // KT):
        ks = pl.ds(kt * KT, KT)
        code = jnp.broadcast_to(code_all[:, kt * KT : (kt + 1) * KT], (R, KT))
        for c in range(GROUPS * I2L):
            mask = jnp.where(code == c, 1.0, 0.0).astype(bf16)
            for j in range(J3):
                y_ref[j, pl.ds(c * R, R), :] = b_ref[pl.ds(j * R, R), ks] * mask
        for j in range(J3):
            q_ref[j, :, ks] = jnp.dot(w_ref[...], y_ref[j], preferred_element_type=f32).astype(bf16)


def first_kernel(row_ref, first_ref, q_ref, out_ref, a_ref, t_ref, o_ref, sem):
    f32, bf16 = jnp.float32, jnp.bfloat16
    blocks = first_ref.shape[0]
    i1 = ((row_ref[...] >> 12) - LEAD) & (blocks - 1)
    hot1 = jnp.where(lax.broadcasted_iota(jnp.int32, (blocks, ROWS), 0) == i1, 1.0, 0.0).astype(bf16)
    a_ref[...] = lax.dot_general(
        first_ref[...], hot1, (((0,), (0,)), ((), ())), preferred_element_type=f32
    )

    def put(kt):
        ks = pl.ds(kt * 128, 128)
        return pltpu.make_async_copy(o_ref.at[ks], out_ref.at[ks], sem.at[kt])

    def tiles(step, carry):
        for u in range(8):
            kt = step * 8 + u
            ks = pl.ds(kt * 128, 128)
            acc = [[None] * J3 for _ in range(J1)]
            for r in range(0, R, 2):
                for j3 in range(J3):
                    both = q_ref[j3, pl.ds(r * J2, 2 * J2), ks].astype(f32)
                    for h in range(2):
                        q = both[h * J2 : (h + 1) * J2]
                        for j1 in range(J1):
                            term = a_ref[pl.ds(j1 * R + r + h, 1), ks] * q
                            acc[j1][j3] = term if acc[j1][j3] is None else acc[j1][j3] + term
            for j1 in range(J1):
                for j3 in range(J3):
                    t_ref[u, pl.ds(j1 * J2 * J3 + j3, J2, stride=J3), :] = acc[j1][j3]
            o_ref[ks, :] = t_ref[u].T.astype(bf16)
            put(kt).start()
        return carry

    tiles(0, 0)
    for kt in range(ROWS // 128):
        put(kt).wait()


def stage_kernel(
    first_hbm, row_hbm, last_hbm, mid_hbm, sent_hbm, row_ref, last_ref, mid_ref, one_ref, many_ref, sems
):
    one = pltpu.make_async_copy(first_hbm, one_ref, sems.at[0])
    others = [
        pltpu.make_async_copy(row_hbm, row_ref, sems.at[1]),
        pltpu.make_async_copy(last_hbm, last_ref, sems.at[2]),
        pltpu.make_async_copy(mid_hbm, mid_ref, sems.at[3]),
    ]
    one.start()
    for copy in others:
        copy.start()
    one.wait()
    many_ref[...] = jnp.broadcast_to(one_ref[...][None], many_ref.shape)
    out = pltpu.make_async_copy(many_ref, sent_hbm, sems.at[4])
    out.start()
    for copy in others:
        copy.wait()
    out.wait()


def stage_call(first_core, row, last_core, mid, blocks):
    far = pl.BlockSpec(memory_space=pltpu.HBM)
    vmem = pl.BlockSpec(memory_space=pltpu.VMEM)
    i32, bf16 = jnp.int32, jnp.bfloat16
    return pl.pallas_call(
        stage_kernel,
        out_shape=(
            pltpu.HBM((blocks, 1, J1 * R), bf16),
            pltpu.VMEM((1, ROWS), i32),
            pltpu.VMEM((R, W3 * J3), bf16),
            pltpu.VMEM((R * I2L, J2 * R), bf16),
        ),
        in_specs=[far] * 4,
        out_specs=(far, vmem, vmem, vmem),
        scratch_shapes=[
            pltpu.VMEM((1, J1 * R), bf16),
            pltpu.VMEM((blocks, 1, J1 * R), bf16),
            pltpu.SemaphoreType.DMA((5,)),
        ],
        compiler_params=pltpu.CompilerParams(vmem_limit_bytes=4 * 1024 * 1024),
        name="stage",
    )(*[pltpu.with_memory_space_constraint(a, pltpu.HBM) for a in (first_core, row, last_core, mid)])


def place_of(block):
    return block // 16, (block // 4) % 4, block % 4


def lateness(block):
    y, _, z = place_of(block)
    return 4 * z + jnp.minimum(y, 8 - y)


def served_rows(first_core, middle_core, last_core, row_tt):
    blocks = lax.axis_size("blk")
    vmem = pl.BlockSpec(memory_space=pltpu.VMEM)
    row = row_tt.reshape(1, ROWS)
    soon = lateness(lax.axis_index("blk")) <= SOON
    zlo = lax.axis_index("sub") // 2
    order = jnp.stack([soon.astype(jnp.int32), zlo.astype(jnp.int32)])
    mid = middle_core.reshape(R * I2L, J2 * R)
    early = [b for b in range(blocks) if 4 * (b % 4) + min(b // 16, 8 - b // 16) <= SOON]
    pairs = [(4 * b + i, 4 * b + (i ^ 2)) for b in early for i in range(4)]
    other = lax.ppermute(mid, ("blk", "sub"), pairs)
    sent, row, last_near, mid_near = stage_call(first_core, row, last_core, mid, blocks)
    ring = [[(p + LEAD) % blocks for p in range(blocks)]]
    first_all = lax.all_to_all(
        sent, "blk", split_axis=0, concat_axis=0, tiled=True, axis_index_groups=ring
    ).reshape(blocks, J1 * R)
    mid_all = lax.cond(soon, from_pair, from_four, mid_near, other)
    q = early_call(order, row, mid_all, last_near, vmem)
    return late_call(row, first_all, q, vmem)


def from_pair(mid, other):
    pair = jnp.concatenate([mid, other], axis=0)
    return lax.all_gather(pair, "sub", axis_index_groups=[[0, 1], [2, 3]], tiled=True)


def from_four(mid, other):
    return lax.all_gather(mid, "sub", tiled=True)


def early_call(order, row, mid_all, last_core, vmem):
    return pl.pallas_call(
        mid_last_kernel,
        out_shape=jax.ShapeDtypeStruct((J3, R * J2, ROWS), jnp.bfloat16),
        in_specs=[pl.BlockSpec(memory_space=pltpu.SMEM), vmem, vmem, vmem],
        out_specs=vmem,
        scratch_shapes=[
            pltpu.VMEM((R * J2, GROUPS * I2L * R), jnp.bfloat16),
            pltpu.VMEM((J3 * R, ROWS), jnp.bfloat16),
            pltpu.VMEM((J3, GROUPS * I2L * R, KT), jnp.bfloat16),
            pltpu.VMEM((2, R * I2L, 128), jnp.float32),
            pltpu.VMEM((2, R * J2, 128), jnp.float32),
        ],
        compiler_params=pltpu.CompilerParams(vmem_limit_bytes=24 * 1024 * 1024),
        name="mid_last",
    )(order, row, mid_all, last_core)


def late_call(row, first_all, q, vmem):
    return pl.pallas_call(
        first_kernel,
        out_shape=jax.ShapeDtypeStruct((ROWS, J1 * J2 * J3), jnp.bfloat16),
        in_specs=[vmem, vmem, vmem],
        out_specs=pl.BlockSpec(memory_space=pl.ANY),
        scratch_shapes=[
            pltpu.VMEM((J1 * R, ROWS), jnp.float32),
            pltpu.VMEM((8, J1 * J2 * J3, 128), jnp.float32),
            pltpu.VMEM((ROWS, J1 * J2 * J3), jnp.bfloat16),
            pltpu.SemaphoreType.DMA((ROWS // 128,)),
        ],
        compiler_params=pltpu.CompilerParams(vmem_limit_bytes=24 * 1024 * 1024),
        name="first",
    )(row, first_all, q)


def solution(mesh):
    placed = (P("blk", None), P(None, "sub", None), P(), P(("blk", "sub")))
    return jax.shard_map(
        served_rows, mesh=mesh, in_specs=placed, out_specs=P(("blk", "sub"), None), check_vma=False
    )
```

```python
import jax
import jax.numpy as jnp
from jax import lax
from jax.experimental import pallas as pl
from jax.experimental.pallas import tpu as pltpu
from jax.sharding import PartitionSpec as P


R = 32
J1 = 4
J2 = 8
J3 = 4
W3 = 128
I2L = 8
GROUPS = 4
ROWS = 1024
KT = 256
LEAD = 17
SOON = 7


def rank_of(block):
    return (((block + 1) & 3) << 5) | (((block >> 2) - LEAD) & 31)


def mid_last_kernel(
    order_ref, row_ref, mid_ref, last_ref, q_ref,
    w_ref, b_ref, y_ref,
):
    f32, bf16 = jnp.float32, jnp.bfloat16
    for t in range(GROUPS):
        w_ref[:, pl.ds(t * 256, 256)] = mid_ref[pl.ds(t * 256, 256), :]
    c_i = lax.broadcasted_iota(jnp.int32, (512, 512), 0)
    d_i = lax.broadcasted_iota(jnp.int32, (512, 512), 1)
    pick = jnp.where(c_i == (d_i & 127) * J3 + (d_i >> 7), 1.0, 0.0).astype(bf16)
    spread = jnp.dot(last_ref[...], pick, preferred_element_type=f32).astype(bf16)
    stacked = jnp.concatenate([spread[:, j * W3 : (j + 1) * W3] for j in range(J3)], axis=0)
    row = row_ref[...]
    i3 = row & (W3 - 1)
    hot3 = jnp.where(lax.broadcasted_iota(jnp.int32, (W3, ROWS), 0) == i3, 1.0, 0.0).astype(bf16)
    b_ref[...] = jnp.dot(stacked, hot3, preferred_element_type=f32).astype(bf16)
    group = (row >> 10) & 3
    paired = ((group & 1) << 1) | ((group >> 1) ^ order_ref[1])
    slot = jnp.where(order_ref[0] == 1, paired, group)
    code_all = slot * I2L + ((row >> 7) & (I2L - 1))
    for kt in range(ROWS // KT):
        ks = pl.ds(kt * KT, KT)
        code = jnp.broadcast_to(code_all[:, kt * KT : (kt + 1) * KT], (R, KT))
        for c in range(GROUPS * I2L):
            mask = jnp.where(code == c, 1.0, 0.0).astype(bf16)
            for j in range(J3):
                y_ref[j, pl.ds(c * R, R), :] = b_ref[pl.ds(j * R, R), ks] * mask
        for j in range(J3):
            q_ref[j, :, ks] = jnp.dot(w_ref[...], y_ref[j], preferred_element_type=f32).astype(bf16)


def first_kernel(row_ref, first_ref, q_ref, out_ref, a_ref, t_ref, o_ref, sem):
    f32, bf16 = jnp.float32, jnp.bfloat16
    blocks = first_ref.shape[0]
    i1 = rank_of(row_ref[...] >> 12)
    hot1 = jnp.where(lax.broadcasted_iota(jnp.int32, (blocks, ROWS), 0) == i1, 1.0, 0.0).astype(bf16)
    a_ref[...] = lax.dot_general(
        first_ref[...], hot1, (((0,), (0,)), ((), ())), preferred_element_type=f32
    )

    def put(kt):
        ks = pl.ds(kt * 128, 128)
        return pltpu.make_async_copy(o_ref.at[ks], out_ref.at[ks], sem.at[kt])

    def tiles(step, carry):
        for u in range(8):
            kt = step * 8 + u
            ks = pl.ds(kt * 128, 128)
            acc = [[None] * J3 for _ in range(J1)]
            for r in range(0, R, 2):
                for j3 in range(J3):
                    both = q_ref[j3, pl.ds(r * J2, 2 * J2), ks].astype(f32)
                    for h in range(2):
                        q = both[h * J2 : (h + 1) * J2]
                        for j1 in range(J1):
                            term = a_ref[pl.ds(j1 * R + r + h, 1), ks] * q
                            acc[j1][j3] = term if acc[j1][j3] is None else acc[j1][j3] + term
            for j1 in range(J1):
                for j3 in range(J3):
                    t_ref[u, pl.ds(j1 * J2 * J3 + j3, J2, stride=J3), :] = acc[j1][j3]
            o_ref[ks, :] = t_ref[u].T.astype(bf16)
            put(kt).start()
        return carry

    tiles(0, 0)
    for kt in range(ROWS // 128):
        put(kt).wait()


def stage_kernel(
    first_hbm, row_hbm, last_hbm, mid_hbm, sent_hbm, row_ref, last_ref, mid_ref,
    one_ref, many_ref, raw_ref, x_ref, v_ref, sems,
):
    one = pltpu.make_async_copy(first_hbm, one_ref, sems.at[0])
    others = [
        pltpu.make_async_copy(row_hbm, row_ref, sems.at[1]),
        pltpu.make_async_copy(last_hbm, last_ref, sems.at[2]),
        pltpu.make_async_copy(mid_hbm, raw_ref, sems.at[3]),
    ]
    one.start()
    for copy in others:
        copy.start()
    one.wait()
    many_ref[...] = jnp.broadcast_to(one_ref[...][None], many_ref.shape)
    out = pltpu.make_async_copy(many_ref, sent_hbm, sems.at[4])
    out.start()
    for copy in others:
        copy.wait()
    chunk = lax.broadcasted_iota(jnp.int32, (R, 128), 1) // R
    for hj in range(2):
        x_ref[hj] = raw_ref[:, pl.ds(hj * 128, 128)].astype(jnp.float32)
    for hi in range(2):
        for hj in range(2):
            turned = []
            for i in range(4):
                v = x_ref[hj, pl.ds(hi * 4 + i, R, stride=I2L), :]
                turned.append([v] + [pltpu.roll(v, R * d, 1) for d in range(1, 4)])
            for j in range(4):
                part = turned[0][(0 - j) % 4]
                for i in range(1, 4):
                    part = jnp.where(chunk == i, turned[i][(i - j) % 4], part)
                v_ref[hi, pl.ds(hj * 4 + j, R, stride=J2), :] = part
    for hi in range(2):
        mid_ref[:, pl.ds(hi * 128, 128)] = v_ref[hi].astype(jnp.bfloat16)
    out.wait()


def stage_call(first_core, row, last_core, mid, blocks):
    far = pl.BlockSpec(memory_space=pltpu.HBM)
    vmem = pl.BlockSpec(memory_space=pltpu.VMEM)
    i32, bf16 = jnp.int32, jnp.bfloat16
    return pl.pallas_call(
        stage_kernel,
        out_shape=(
            pltpu.HBM((blocks, 1, J1 * R), bf16),
            pltpu.VMEM((1, ROWS), i32),
            pltpu.VMEM((R, W3 * J3), bf16),
            pltpu.VMEM((R * I2L, J2 * R), bf16),
        ),
        in_specs=[far] * 4,
        out_specs=(far, vmem, vmem, vmem),
        scratch_shapes=[
            pltpu.VMEM((1, J1 * R), bf16),
            pltpu.VMEM((blocks, 1, J1 * R), bf16),
            pltpu.VMEM((R * I2L, J2 * R), bf16),
            pltpu.VMEM((2, R * I2L, 128), jnp.float32),
            pltpu.VMEM((2, R * J2, 128), jnp.float32),
            pltpu.SemaphoreType.DMA((5,)),
        ],
        compiler_params=pltpu.CompilerParams(vmem_limit_bytes=4 * 1024 * 1024),
        name="stage",
    )(*[pltpu.with_memory_space_constraint(a, pltpu.HBM) for a in (first_core, row, last_core, mid)])


def place_of(block):
    return block // 16, (block // 4) % 4, block % 4


def lateness(block):
    y, _, z = place_of(block)
    return 4 * z + jnp.minimum(y, 8 - y)


def served_rows(first_core, middle_core, last_core, row_tt):
    blocks = lax.axis_size("blk")
    vmem = pl.BlockSpec(memory_space=pltpu.VMEM)
    row = row_tt.reshape(1, ROWS)
    soon = lateness(lax.axis_index("blk")) <= SOON
    zlo = lax.axis_index("sub") // 2
    order = jnp.stack([soon.astype(jnp.int32), zlo.astype(jnp.int32)])
    mid = middle_core.reshape(R * I2L, J2 * R)
    early = [b for b in range(blocks) if 4 * (b % 4) + min(b // 16, 8 - b // 16) <= SOON]
    pairs = [(4 * b + i, 4 * b + (i ^ 2)) for b in early for i in range(4)]
    sent, row, last_near, mid_near = stage_call(first_core, row, last_core, mid, blocks)
    other = lax.ppermute(mid_near, ("blk", "sub"), pairs)
    ring = [sorted(range(blocks), key=rank_of)]
    first_all = lax.all_to_all(
        sent, "blk", split_axis=0, concat_axis=0, tiled=True, axis_index_groups=ring
    ).reshape(blocks, J1 * R)
    mid_all = lax.cond(soon, from_pair, from_four, mid_near, other)
    q = early_call(order, row, mid_all, last_near, vmem)
    return late_call(row, first_all, q, vmem)


def from_pair(mid, other):
    pair = jnp.concatenate([mid, other], axis=0)
    return lax.all_gather(pair, "sub", axis_index_groups=[[0, 1], [2, 3]], tiled=True)


def from_four(mid, other):
    return lax.all_gather(mid, "sub", tiled=True)


def early_call(order, row, mid_all, last_core, vmem):
    return pl.pallas_call(
        mid_last_kernel,
        out_shape=jax.ShapeDtypeStruct((J3, R * J2, ROWS), jnp.bfloat16),
        in_specs=[pl.BlockSpec(memory_space=pltpu.SMEM), vmem, vmem, vmem],
        out_specs=vmem,
        scratch_shapes=[
            pltpu.VMEM((R * J2, GROUPS * I2L * R), jnp.bfloat16),
            pltpu.VMEM((J3 * R, ROWS), jnp.bfloat16),
            pltpu.VMEM((J3, GROUPS * I2L * R, KT), jnp.bfloat16),
        ],
        compiler_params=pltpu.CompilerParams(vmem_limit_bytes=24 * 1024 * 1024),
        name="mid_last",
    )(order, row, mid_all, last_core)


def late_call(row, first_all, q, vmem):
    return pl.pallas_call(
        first_kernel,
        out_shape=jax.ShapeDtypeStruct((ROWS, J1 * J2 * J3), jnp.bfloat16),
        in_specs=[vmem, vmem, vmem],
        out_specs=pl.BlockSpec(memory_space=pl.ANY),
        scratch_shapes=[
            pltpu.VMEM((J1 * R, ROWS), jnp.float32),
            pltpu.VMEM((8, J1 * J2 * J3, 128), jnp.float32),
            pltpu.VMEM((ROWS, J1 * J2 * J3), jnp.bfloat16),
            pltpu.SemaphoreType.DMA((ROWS // 128,)),
        ],
        compiler_params=pltpu.CompilerParams(vmem_limit_bytes=24 * 1024 * 1024),
        name="first",
    )(row, first_all, q)


def solution(mesh):
    placed = (P("blk", None), P(None, "sub", None), P(), P(("blk", "sub")))
    return jax.shard_map(
        served_rows, mesh=mesh, in_specs=placed, out_specs=P(("blk", "sub"), None), check_vma=False
    )
```

```python
import jax
import jax.numpy as jnp
from jax import lax
from jax.experimental import pallas as pl
from jax.experimental.pallas import tpu as pltpu
from jax.sharding import PartitionSpec as P


R = 32
J1 = 4
J2 = 8
J3 = 4
W3 = 128
I2L = 8
GROUPS = 4
ROWS = 1024
KT = 256
LEAD = 17
SOON = 7


def rank_of(block):
    return (((block + 1) & 3) << 5) | (((block >> 2) - LEAD) & 31)


def mid_last_kernel(
    order_ref, row_ref, mid_ref, last_ref, q_ref,
    w_ref, b_ref, y_ref,
):
    f32, bf16 = jnp.float32, jnp.bfloat16
    for t in range(GROUPS):
        w_ref[:, pl.ds(t * 256, 256)] = mid_ref[pl.ds(t * 256, 256), :]
    row = row_ref[...]
    i3 = row & (W3 - 1)
    hot3 = jnp.where(lax.broadcasted_iota(jnp.int32, (W3, ROWS), 0) == i3, 1.0, 0.0).astype(bf16)
    b_ref[...] = jnp.dot(last_ref[...], hot3, preferred_element_type=f32).astype(bf16)
    group = (row >> 10) & 3
    paired = ((group & 1) << 1) | ((group >> 1) ^ order_ref[1])
    slot = jnp.where(order_ref[0] == 1, paired, group)
    code_all = slot * I2L + ((row >> 7) & (I2L - 1))
    for kt in range(ROWS // KT):
        ks = pl.ds(kt * KT, KT)
        code = jnp.broadcast_to(code_all[:, kt * KT : (kt + 1) * KT], (R, KT))
        for c in range(GROUPS * I2L):
            mask = jnp.where(code == c, 1.0, 0.0).astype(bf16)
            for j in range(J3):
                y_ref[j, pl.ds(c * R, R), :] = b_ref[pl.ds(j * R, R), ks] * mask
        for j in range(J3):
            q_ref[j, :, ks] = jnp.dot(w_ref[...], y_ref[j], preferred_element_type=f32).astype(bf16)


def first_kernel(row_ref, first_ref, q_ref, out_ref, a_ref, t_ref, o_ref, sem):
    f32, bf16 = jnp.float32, jnp.bfloat16
    blocks = first_ref.shape[0]
    i1 = rank_of(row_ref[...] >> 12)
    hot1 = jnp.where(lax.broadcasted_iota(jnp.int32, (blocks, ROWS), 0) == i1, 1.0, 0.0).astype(bf16)
    a_ref[...] = lax.dot_general(
        first_ref[...], hot1, (((0,), (0,)), ((), ())), preferred_element_type=f32
    )

    def put(kt):
        ks = pl.ds(kt * 128, 128)
        return pltpu.make_async_copy(o_ref.at[ks], out_ref.at[ks], sem.at[kt])

    def tiles(step, carry):
        for u in range(8):
            kt = step * 8 + u
            ks = pl.ds(kt * 128, 128)
            acc = [[None] * J3 for _ in range(J1)]
            for r in range(0, R, 2):
                for j3 in range(J3):
                    both = q_ref[j3, pl.ds(r * J2, 2 * J2), ks].astype(f32)
                    for h in range(2):
                        q = both[h * J2 : (h + 1) * J2]
                        for j1 in range(J1):
                            term = a_ref[pl.ds(j1 * R + r + h, 1), ks] * q
                            acc[j1][j3] = term if acc[j1][j3] is None else acc[j1][j3] + term
            for j1 in range(J1):
                for j3 in range(J3):
                    t_ref[u, pl.ds(j1 * J2 * J3 + j3, J2, stride=J3), :] = acc[j1][j3]
            o_ref[ks, :] = t_ref[u].T.astype(bf16)
            put(kt).start()
        return carry

    tiles(0, 0)
    for kt in range(ROWS // 128):
        put(kt).wait()


def stage_kernel(
    first_hbm, row_hbm, last_hbm, mid_hbm, sent_hbm, row_ref, last_ref, mid_ref,
    one_ref, many_ref, raw_ref, raw_last_ref, pick_ref, x_ref, v_ref, sems,
):
    one = pltpu.make_async_copy(first_hbm, one_ref, sems.at[0])
    others = [
        pltpu.make_async_copy(row_hbm, row_ref, sems.at[1]),
        pltpu.make_async_copy(last_hbm, raw_last_ref, sems.at[2]),
        pltpu.make_async_copy(mid_hbm, raw_ref, sems.at[3]),
    ]
    one.start()
    for copy in others:
        copy.start()
    c_i = lax.broadcasted_iota(jnp.int32, (W3 * J3, W3 * J3), 0)
    d_i = lax.broadcasted_iota(jnp.int32, (W3 * J3, W3 * J3), 1)
    pick_ref[...] = jnp.where(c_i == (d_i & (W3 - 1)) * J3 + d_i // W3, 1.0, 0.0).astype(jnp.bfloat16)
    one.wait()
    many_ref[...] = jnp.broadcast_to(one_ref[...][None], many_ref.shape)
    out = pltpu.make_async_copy(many_ref, sent_hbm, sems.at[4])
    out.start()
    for copy in others:
        copy.wait()
    spread = jnp.dot(raw_last_ref[...], pick_ref[...], preferred_element_type=jnp.float32)
    for j in range(J3):
        last_ref[pl.ds(j * R, R), :] = spread[:, j * W3 : (j + 1) * W3].astype(jnp.bfloat16)
    chunk = lax.broadcasted_iota(jnp.int32, (R, 128), 1) // R
    for hj in range(2):
        x_ref[hj] = raw_ref[:, pl.ds(hj * 128, 128)].astype(jnp.float32)
    for hi in range(2):
        for hj in range(2):
            turned = []
            for i in range(4):
                v = x_ref[hj, pl.ds(hi * 4 + i, R, stride=I2L), :]
                turned.append([v] + [pltpu.roll(v, R * d, 1) for d in range(1, 4)])
            for j in range(4):
                part = turned[0][(0 - j) % 4]
                for i in range(1, 4):
                    part = jnp.where(chunk == i, turned[i][(i - j) % 4], part)
                v_ref[hi, pl.ds(hj * 4 + j, R, stride=J2), :] = part
    for hi in range(2):
        mid_ref[:, pl.ds(hi * 128, 128)] = v_ref[hi].astype(jnp.bfloat16)
    out.wait()


def stage_call(first_core, row, last_core, mid, blocks):
    far = pl.BlockSpec(memory_space=pltpu.HBM)
    vmem = pl.BlockSpec(memory_space=pltpu.VMEM)
    i32, bf16 = jnp.int32, jnp.bfloat16
    return pl.pallas_call(
        stage_kernel,
        out_shape=(
            pltpu.HBM((blocks, 1, J1 * R), bf16),
            pltpu.VMEM((1, ROWS), i32),
            pltpu.VMEM((J3 * R, W3), bf16),
            pltpu.VMEM((R * I2L, J2 * R), bf16),
        ),
        in_specs=[far] * 4,
        out_specs=(far, vmem, vmem, vmem),
        scratch_shapes=[
            pltpu.VMEM((1, J1 * R), bf16),
            pltpu.VMEM((blocks, 1, J1 * R), bf16),
            pltpu.VMEM((R * I2L, J2 * R), bf16),
            pltpu.VMEM((R, W3 * J3), bf16),
            pltpu.VMEM((W3 * J3, W3 * J3), bf16),
            pltpu.VMEM((2, R * I2L, 128), jnp.float32),
            pltpu.VMEM((2, R * J2, 128), jnp.float32),
            pltpu.SemaphoreType.DMA((5,)),
        ],
        compiler_params=pltpu.CompilerParams(vmem_limit_bytes=4 * 1024 * 1024),
        name="stage",
    )(*[pltpu.with_memory_space_constraint(a, pltpu.HBM) for a in (first_core, row, last_core, mid)])


def place_of(block):
    return block // 16, (block // 4) % 4, block % 4


def lateness(block):
    y, _, z = place_of(block)
    return 4 * z + jnp.minimum(y, 8 - y)


def served_rows(first_core, middle_core, last_core, row_tt):
    blocks = lax.axis_size("blk")
    vmem = pl.BlockSpec(memory_space=pltpu.VMEM)
    row = row_tt.reshape(1, ROWS)
    soon = lateness(lax.axis_index("blk")) <= SOON
    zlo = lax.axis_index("sub") // 2
    order = jnp.stack([soon.astype(jnp.int32), zlo.astype(jnp.int32)])
    mid = middle_core.reshape(R * I2L, J2 * R)
    early = [b for b in range(blocks) if 4 * (b % 4) + min(b // 16, 8 - b // 16) <= SOON]
    pairs = [(4 * b + i, 4 * b + (i ^ 2)) for b in early for i in range(4)]
    sent, row, last_near, mid_near = stage_call(first_core, row, last_core, mid, blocks)
    other = lax.ppermute(mid_near, ("blk", "sub"), pairs)
    ring = [sorted(range(blocks), key=rank_of)]
    first_all = lax.all_to_all(
        sent, "blk", split_axis=0, concat_axis=0, tiled=True, axis_index_groups=ring
    ).reshape(blocks, J1 * R)
    mid_all = lax.cond(soon, from_pair, from_four, mid_near, other)
    q = early_call(order, row, mid_all, last_near, vmem)
    return late_call(row, first_all, q, vmem)


def from_pair(mid, other):
    pair = jnp.concatenate([mid, other], axis=0)
    return lax.all_gather(pair, "sub", axis_index_groups=[[0, 1], [2, 3]], tiled=True)


def from_four(mid, other):
    return lax.all_gather(mid, "sub", tiled=True)


def early_call(order, row, mid_all, last_core, vmem):
    return pl.pallas_call(
        mid_last_kernel,
        out_shape=jax.ShapeDtypeStruct((J3, R * J2, ROWS), jnp.bfloat16),
        in_specs=[pl.BlockSpec(memory_space=pltpu.SMEM), vmem, vmem, vmem],
        out_specs=vmem,
        scratch_shapes=[
            pltpu.VMEM((R * J2, GROUPS * I2L * R), jnp.bfloat16),
            pltpu.VMEM((J3 * R, ROWS), jnp.bfloat16),
            pltpu.VMEM((J3, GROUPS * I2L * R, KT), jnp.bfloat16),
        ],
        compiler_params=pltpu.CompilerParams(vmem_limit_bytes=24 * 1024 * 1024),
        name="mid_last",
    )(order, row, mid_all, last_core)


def late_call(row, first_all, q, vmem):
    return pl.pallas_call(
        first_kernel,
        out_shape=jax.ShapeDtypeStruct((ROWS, J1 * J2 * J3), jnp.bfloat16),
        in_specs=[vmem, vmem, vmem],
        out_specs=pl.BlockSpec(memory_space=pl.ANY),
        scratch_shapes=[
            pltpu.VMEM((J1 * R, ROWS), jnp.float32),
            pltpu.VMEM((8, J1 * J2 * J3, 128), jnp.float32),
            pltpu.VMEM((ROWS, J1 * J2 * J3), jnp.bfloat16),
            pltpu.SemaphoreType.DMA((ROWS // 128,)),
        ],
        compiler_params=pltpu.CompilerParams(vmem_limit_bytes=24 * 1024 * 1024),
        name="first",
    )(row, first_all, q)


def solution(mesh):
    placed = (P("blk", None), P(None, "sub", None), P(), P(("blk", "sub")))
    return jax.shard_map(
        served_rows, mesh=mesh, in_specs=placed, out_specs=P(("blk", "sub"), None), check_vma=False
    )
```

```python
import jax
import jax.numpy as jnp
from jax import lax
from jax.experimental import pallas as pl
from jax.experimental.pallas import tpu as pltpu
from jax.sharding import PartitionSpec as P


R = 32
J1 = 4
J2 = 8
J3 = 4
W3 = 128
I2L = 8
GROUPS = 4
ROWS = 1024
KT = 256
LEAD = 17
SOON = 7


def rank_of(block):
    return (((block + 1) & 3) << 5) | (((block >> 2) - LEAD) & 31)


def mid_last_kernel(
    order_ref, row_ref, mid_ref, last_ref, q_ref,
    w_ref, b_ref, y_ref,
):
    f32, bf16 = jnp.float32, jnp.bfloat16
    for t in range(GROUPS):
        w_ref[:, pl.ds(t * 256, 256)] = mid_ref[pl.ds(t * 256, 256), :]
    row = row_ref[...]
    i3 = row & (W3 - 1)
    hot3 = jnp.where(lax.broadcasted_iota(jnp.int32, (W3, ROWS), 0) == i3, 1.0, 0.0).astype(bf16)
    b_ref[...] = jnp.dot(last_ref[...], hot3, preferred_element_type=f32).astype(bf16)
    group = (row >> 10) & 3
    paired = ((group & 1) << 1) | ((group >> 1) ^ order_ref[1:2, :])
    slot = jnp.where(order_ref[0:1, :] == 1, paired, group)
    code_all = slot * I2L + ((row >> 7) & (I2L - 1))
    for kt in range(ROWS // KT):
        ks = pl.ds(kt * KT, KT)
        code = jnp.broadcast_to(code_all[:, kt * KT : (kt + 1) * KT], (R, KT))
        for c in range(GROUPS * I2L):
            mask = jnp.where(code == c, 1.0, 0.0).astype(bf16)
            for j in range(J3):
                y_ref[j, pl.ds(c * R, R), :] = b_ref[pl.ds(j * R, R), ks] * mask
        for j in range(J3):
            q_ref[j, :, ks] = jnp.dot(w_ref[...], y_ref[j], preferred_element_type=f32).astype(bf16)


def first_kernel(row_ref, first_ref, q_ref, out_ref, a_ref, t_ref, o_ref, sem):
    f32, bf16 = jnp.float32, jnp.bfloat16
    blocks = first_ref.shape[0]
    i1 = rank_of(row_ref[...] >> 12)
    hot1 = jnp.where(lax.broadcasted_iota(jnp.int32, (blocks, ROWS), 0) == i1, 1.0, 0.0).astype(bf16)
    a_ref[...] = lax.dot_general(
        first_ref[...], hot1, (((0,), (0,)), ((), ())), preferred_element_type=f32
    )

    def put(kt):
        ks = pl.ds(kt * 128, 128)
        return pltpu.make_async_copy(o_ref.at[ks], out_ref.at[ks], sem.at[kt])

    def tiles(step, carry):
        for u in range(8):
            kt = step * 8 + u
            ks = pl.ds(kt * 128, 128)
            acc = [[None] * J3 for _ in range(J1)]
            for r in range(0, R, 2):
                for j3 in range(J3):
                    both = q_ref[j3, pl.ds(r * J2, 2 * J2), ks].astype(f32)
                    for h in range(2):
                        q = both[h * J2 : (h + 1) * J2]
                        for j1 in range(J1):
                            term = a_ref[pl.ds(j1 * R + r + h, 1), ks] * q
                            acc[j1][j3] = term if acc[j1][j3] is None else acc[j1][j3] + term
            for j1 in range(J1):
                for j3 in range(J3):
                    t_ref[u, pl.ds(j1 * J2 * J3 + j3, J2, stride=J3), :] = acc[j1][j3]
            o_ref[ks, :] = t_ref[u].T.astype(bf16)
            put(kt).start()
        return carry

    tiles(0, 0)
    for kt in range(ROWS // 128):
        put(kt).wait()


def stage_kernel(
    first_hbm, row_hbm, last_hbm, mid_hbm, sent_hbm, row_ref, last_ref, mid_ref,
    one_ref, many_ref, raw_ref, raw_last_ref, pick_ref, x_ref, v_ref, sems,
):
    one = pltpu.make_async_copy(first_hbm, one_ref, sems.at[0])
    others = [
        pltpu.make_async_copy(row_hbm, row_ref, sems.at[1]),
        pltpu.make_async_copy(last_hbm, raw_last_ref, sems.at[2]),
        pltpu.make_async_copy(mid_hbm, raw_ref, sems.at[3]),
    ]
    one.start()
    for copy in others:
        copy.start()
    c_i = lax.broadcasted_iota(jnp.int32, (W3 * J3, W3 * J3), 0)
    d_i = lax.broadcasted_iota(jnp.int32, (W3 * J3, W3 * J3), 1)
    pick_ref[...] = jnp.where(c_i == (d_i & (W3 - 1)) * J3 + d_i // W3, 1.0, 0.0).astype(jnp.bfloat16)
    one.wait()
    many_ref[...] = jnp.broadcast_to(one_ref[...][None], many_ref.shape)
    out = pltpu.make_async_copy(many_ref, sent_hbm, sems.at[4])
    out.start()
    for copy in others:
        copy.wait()
    spread = jnp.dot(raw_last_ref[...], pick_ref[...], preferred_element_type=jnp.float32)
    for j in range(J3):
        last_ref[pl.ds(j * R, R), :] = spread[:, j * W3 : (j + 1) * W3].astype(jnp.bfloat16)
    chunk = lax.broadcasted_iota(jnp.int32, (R, 128), 1) // R
    for hj in range(2):
        x_ref[hj] = raw_ref[:, pl.ds(hj * 128, 128)].astype(jnp.float32)
    for hi in range(2):
        for hj in range(2):
            turned = []
            for i in range(4):
                v = x_ref[hj, pl.ds(hi * 4 + i, R, stride=I2L), :]
                turned.append([v] + [pltpu.roll(v, R * d, 1) for d in range(1, 4)])
            for j in range(4):
                part = turned[0][(0 - j) % 4]
                for i in range(1, 4):
                    part = jnp.where(chunk == i, turned[i][(i - j) % 4], part)
                v_ref[hi, pl.ds(hj * 4 + j, R, stride=J2), :] = part
    for hi in range(2):
        mid_ref[:, pl.ds(hi * 128, 128)] = v_ref[hi].astype(jnp.bfloat16)
    out.wait()


def stage_call(first_core, row, last_core, mid, blocks):
    far = pl.BlockSpec(memory_space=pltpu.HBM)
    vmem = pl.BlockSpec(memory_space=pltpu.VMEM)
    i32, bf16 = jnp.int32, jnp.bfloat16
    return pl.pallas_call(
        stage_kernel,
        out_shape=(
            pltpu.HBM((blocks, 1, J1 * R), bf16),
            pltpu.VMEM((1, ROWS), i32),
            pltpu.VMEM((J3 * R, W3), bf16),
            pltpu.VMEM((R * I2L, J2 * R), bf16),
        ),
        in_specs=[far] * 4,
        out_specs=(far, vmem, vmem, vmem),
        scratch_shapes=[
            pltpu.VMEM((1, J1 * R), bf16),
            pltpu.VMEM((blocks, 1, J1 * R), bf16),
            pltpu.VMEM((R * I2L, J2 * R), bf16),
            pltpu.VMEM((R, W3 * J3), bf16),
            pltpu.VMEM((W3 * J3, W3 * J3), bf16),
            pltpu.VMEM((2, R * I2L, 128), jnp.float32),
            pltpu.VMEM((2, R * J2, 128), jnp.float32),
            pltpu.SemaphoreType.DMA((5,)),
        ],
        compiler_params=pltpu.CompilerParams(vmem_limit_bytes=4 * 1024 * 1024),
        name="stage",
    )(*[pltpu.with_memory_space_constraint(a, pltpu.HBM) for a in (first_core, row, last_core, mid)])


def place_of(block):
    return block // 16, (block // 4) % 4, block % 4


def lateness(block):
    y, _, z = place_of(block)
    return 4 * z + jnp.minimum(y, 8 - y)


def served_rows(first_core, middle_core, last_core, row_tt):
    blocks = lax.axis_size("blk")
    vmem = pl.BlockSpec(memory_space=pltpu.VMEM)
    row = row_tt.reshape(1, ROWS)
    soon = lateness(lax.axis_index("blk")) <= SOON
    zlo = lax.axis_index("sub") // 2
    order = jnp.stack([soon.astype(jnp.int32), zlo.astype(jnp.int32)])
    order = jnp.broadcast_to(order[:, None], (2, ROWS))
    mid = middle_core.reshape(R * I2L, J2 * R)
    early = [b for b in range(blocks) if 4 * (b % 4) + min(b // 16, 8 - b // 16) <= SOON]
    pairs = [(4 * b + i, 4 * b + (i ^ 2)) for b in early for i in range(4)]
    sent, row, last_near, mid_near = stage_call(first_core, row, last_core, mid, blocks)
    other = lax.ppermute(mid_near, ("blk", "sub"), pairs)
    ring = [sorted(range(blocks), key=rank_of)]
    first_all = lax.all_to_all(
        sent, "blk", split_axis=0, concat_axis=0, tiled=True, axis_index_groups=ring
    ).reshape(blocks, J1 * R)
    mid_all = lax.cond(soon, from_pair, from_four, mid_near, other)
    q = early_call(order, row, mid_all, last_near, vmem)
    return late_call(row, first_all, q, vmem)


def from_pair(mid, other):
    pair = jnp.concatenate([mid, other], axis=0)
    return lax.all_gather(pair, "sub", axis_index_groups=[[0, 1], [2, 3]], tiled=True)


def from_four(mid, other):
    return lax.all_gather(mid, "sub", tiled=True)


def early_call(order, row, mid_all, last_core, vmem):
    return pl.pallas_call(
        mid_last_kernel,
        out_shape=jax.ShapeDtypeStruct((J3, R * J2, ROWS), jnp.bfloat16),
        in_specs=[vmem, vmem, vmem, vmem],
        out_specs=vmem,
        scratch_shapes=[
            pltpu.VMEM((R * J2, GROUPS * I2L * R), jnp.bfloat16),
            pltpu.VMEM((J3 * R, ROWS), jnp.bfloat16),
            pltpu.VMEM((J3, GROUPS * I2L * R, KT), jnp.bfloat16),
        ],
        compiler_params=pltpu.CompilerParams(vmem_limit_bytes=24 * 1024 * 1024),
        name="mid_last",
    )(order, row, mid_all, last_core)


def late_call(row, first_all, q, vmem):
    return pl.pallas_call(
        first_kernel,
        out_shape=jax.ShapeDtypeStruct((ROWS, J1 * J2 * J3), jnp.bfloat16),
        in_specs=[vmem, vmem, vmem],
        out_specs=pl.BlockSpec(memory_space=pl.ANY),
        scratch_shapes=[
            pltpu.VMEM((J1 * R, ROWS), jnp.float32),
            pltpu.VMEM((8, J1 * J2 * J3, 128), jnp.float32),
            pltpu.VMEM((ROWS, J1 * J2 * J3), jnp.bfloat16),
            pltpu.SemaphoreType.DMA((ROWS // 128,)),
        ],
        compiler_params=pltpu.CompilerParams(vmem_limit_bytes=24 * 1024 * 1024),
        name="first",
    )(row, first_all, q)


def solution(mesh):
    placed = (P("blk", None), P(None, "sub", None), P(), P(("blk", "sub")))
    return jax.shard_map(
        served_rows, mesh=mesh, in_specs=placed, out_specs=P(("blk", "sub"), None), check_vma=False
    )
```
